256 devices in a mesh: leaf: 16 (over z, core), pts: 16 (over x, y).
Axes of the slice: x: 4, y: 4, z: 8, core: 2. Of those that a mesh axis runs over, the one named last changes fastest.
Arguments:
- leaf_solved: float32 [262144, 256], P(('leaf', 'pts')), may hold values from -6 to 6
- points: float32 [3, 262144], P(None, ('leaf', 'pts')), may hold values from -8 to 8
- panel_top: float32 [262144, 256], P(('leaf', 'pts')), may hold values from -0.015625 to 0.015625
- panel_mid: float32 [262144, 256], P(('leaf', 'pts')), may hold values from -0.0234375 to 0.0234375
- panel_low: float32 [262144, 256], P(('leaf', 'pts')), may hold values from -0.03125 to 0.03125
- solved_top: float32 [262144, 256], P(('leaf', 'pts')), may hold values from -0.046875 to 0.046875
- solved_mid: float32 [262144, 256], P(('leaf', 'pts')), may hold values from -0.046875 to 0.046875
- solved_low: float32 [262144, 256], P(('leaf', 'pts')), may hold values from -0.046875 to 0.046875
- skeleton_top: int32 [2, 256], replicated, may hold values from 0 to 262143, as said below
- skeleton_mid: int32 [4, 256], replicated, may hold values from 0 to 262143, as said below
- skeleton_low: int32 [8, 256], replicated, may hold values from 0 to 262143, as said below
Outputs:
- solution: float32 [262144, 256], P(('leaf', 'pts'))
The draws below stay inside these ranges and needn't reach their ends.
Inputs may be any that keep to these rules, and one draw needn't show every extreme that they name: `skeleton_top`: row k holds 256 different indices of points of child k of the level, all between k * 131072 and (k + 1) * 131072 - 1. `skeleton_mid`: row k holds 256 different indices of points of child k of the level, all between k * 65536 and (k + 1) * 65536 - 1. `skeleton_low`: row k holds 256 different indices of points of child k of the level, all between k * 32768 and (k + 1) * 32768 - 1.
All inputs are finite; a program needn't handle non-finite values.
Results may differ from the reference program's by a relative error of at most 0.00005.
Values sent between devices are 32-bit elements; how exact they have to be, the bound alone decides.
No kernel may reach another device: no remote copies, remote signals or barrier semaphores. Data moves between devices by JAX's collectives and lax.ppermute only.
A program may use at most 128 MiB of HBM per device.

```python
import jax
import jax.numpy as jnp
from jax import lax

R = 256
NRHS = 256
N = 262144


def skeleton_draw(key, count):
    size = N // count
    child_keys = jax.random.split(key, count)

    def one_child(child_key):
        return jax.random.permutation(child_key, size)[:R].astype(jnp.int32)
    chosen = jax.vmap(one_child)(child_keys)
    return chosen + jnp.arange(count, dtype=jnp.int32)[:, None] * size


def draw_skeleton_top(key, part):
    return skeleton_draw(jax.random.fold_in(key, 11), 2)


def draw_skeleton_mid(key, part):
    return skeleton_draw(jax.random.fold_in(key, 12), 4)


def draw_skeleton_low(key, part):
    return skeleton_draw(jax.random.fold_in(key, 13), 8)


def level_of(stream_key, shape, cuts, low, largest):
    factor_of = 1.0
    for axis_at, shards_of in cuts:
        steps = jax.random.uniform(jax.random.fold_in(jax.random.fold_in(stream_key, 6), axis_at), (shards_of,), jnp.float32, low / len(cuts), largest / len(cuts))
        factor_of = factor_of * jnp.repeat(jnp.exp(steps), shape[axis_at] // shards_of).reshape((-1,) + (1,) * (len(shape) - 1 - axis_at))
    return factor_of


def gaussian(own_key, dims, scale, bound, cuts=(), kind=jnp.bfloat16):
    array = scale * jax.random.normal(own_key, dims, jnp.float32)
    if cuts:
        array = array * level_of(own_key, dims, cuts, -0.22, 0.18)
    return jnp.clip(array, -bound, bound).astype(kind)


def setup_inputs(seed: int = 0) -> dict:
    splits = jax.random.split(jax.random.key(seed), 12)
    leaf_solved = gaussian(splits[0], (N, NRHS), 1.0, 6.0, ((0, 256),), jnp.float32)
    points = jnp.clip(jax.random.uniform(splits[1], (3, N), jnp.float32, -8.0, 8.0) * level_of(splits[1], (3, N), ((1, 256),), -0.4, 0.0), -8.0, 8.0)
    panel_top = gaussian(splits[2], (N, R), (N // 2) ** -0.5, 0.015625, ((0, 256),), jnp.float32)
    panel_mid = gaussian(splits[3], (N, R), (N // 4) ** -0.5, 0.0234375, ((0, 256),), jnp.float32)
    panel_low = gaussian(splits[4], (N, R), (N // 8) ** -0.5, 0.03125, ((0, 256),), jnp.float32)
    solved_top = gaussian(splits[5], (N, R), (64 * R) ** -0.5, 0.046875, ((0, 256),), jnp.float32)
    solved_mid = gaussian(splits[6], (N, R), (64 * R) ** -0.5, 0.046875, ((0, 256),), jnp.float32)
    solved_low = gaussian(splits[7], (N, R), (64 * R) ** -0.5, 0.046875, ((0, 256),), jnp.float32)
    skeleton_top = draw_skeleton_top(jax.random.fold_in(splits[11], 71), 0)
    skeleton_mid = draw_skeleton_mid(jax.random.fold_in(splits[11], 71), 0)
    skeleton_low = draw_skeleton_low(jax.random.fold_in(splits[11], 71), 0)
    return {"leaf_solved": leaf_solved, "points": points, "panel_top": panel_top, "panel_mid": panel_mid, "panel_low": panel_low, "solved_top": solved_top, "solved_mid": solved_mid, "solved_low": solved_low, "skeleton_top": skeleton_top, "skeleton_mid": skeleton_mid, "skeleton_low": skeleton_low}


HIGH = lax.Precision.HIGHEST

def kernel_block(lower, upper):
    spread = lower[:, :, None] - upper[:, None, :]
    return jnp.exp(-0.5 * jnp.sum(spread * spread, axis=0))

def pair_solve(gram_pair, proj_pair, spot_pair):
    rank = gram_pair.shape[1]
    couple = kernel_block(spot_pair[:, 0], spot_pair[:, 1])
    ident = jnp.eye(rank, dtype=jnp.float32)
    upper_right = jnp.dot(couple, gram_pair[1], precision=HIGH)
    lower_left = jnp.dot(couple.T, gram_pair[0], precision=HIGH)
    system = jnp.concatenate([jnp.concatenate([ident, upper_right], 1), jnp.concatenate([lower_left, ident], 1)], 0)
    target = jnp.concatenate([jnp.dot(couple, proj_pair[1], precision=HIGH), jnp.dot(couple.T, proj_pair[0], precision=HIGH)], 0)
    answer = jnp.linalg.solve(system, target)
    return answer.reshape(2, rank, -1)

def level_solve(carry, panel, skeleton, points):
    count = skeleton.shape[0]
    rank = panel.shape[1]
    total = carry.shape[0]
    size = total // count
    current = carry[:, total * 0 + carry.shape[1] - rank:].reshape(count, size, rank)
    rest = carry[:, :carry.shape[1] - rank].reshape(count, size, -1)
    blocks = panel.reshape(count, size, rank)
    gram = jnp.einsum('cnr,cns->crs', blocks, current, precision=HIGH)
    proj = jnp.einsum('cnr,cnk->crk', blocks, rest, precision=HIGH)
    spots = points[:, skeleton.reshape(-1).astype(jnp.int32)].reshape(3, count // 2, 2, rank)
    spots = jnp.transpose(spots, (1, 0, 2, 3))
    answers = jax.vmap(pair_solve)(gram.reshape(count // 2, 2, rank, rank), proj.reshape(count // 2, 2, rank, -1), spots)
    answers = answers.reshape(count, rank, -1)
    rest = rest - jnp.einsum('cnr,crk->cnk', current, answers, precision=HIGH)
    return rest.reshape(total, -1)

def reference(leaf_solved, points, panel_top, panel_mid, panel_low, solved_top, solved_mid, solved_low, skeleton_top, skeleton_mid, skeleton_low):
    carry = jnp.concatenate([leaf_solved, solved_top, solved_mid, solved_low], axis=1)
    carry = level_solve(carry, panel_low, skeleton_low, points)
    carry = level_solve(carry, panel_mid, skeleton_mid, points)
    return level_solve(carry, panel_top, skeleton_top, points)
```

```python
import functools

import jax
import jax.numpy as jnp
from jax import lax
from jax.experimental import pallas as pl
from jax.experimental.pallas import tpu as pltpu
from jax.sharding import PartitionSpec as P

F32 = jnp.float32
HIGH = lax.Precision.HIGH
BEST = lax.Precision.HIGHEST


def mm(a, b):
    return jnp.dot(a, b, precision=BEST, preferred_element_type=F32)


def mm_t(a, b):
    return lax.dot_general(
        a, b, (((1,), (1,)), ((), ())), precision=BEST, preferred_element_type=F32
    )


def fro2(value):
    return jnp.sum(value * value)


def inverse_into(n_ref, y_ref, e_ref):
    rank = n_ref.shape[0]
    row = lax.broadcasted_iota(jnp.int32, (rank, rank), 0)
    col = lax.broadcasted_iota(jnp.int32, (rank, rank), 1)
    ident = jnp.where(row == col, 1.0, 0.0).astype(F32)
    y_ref[...] = ident + n_ref[...]
    e_ref[...] = n_ref[...]

    @pl.loop(0, 3)
    def _(step):
        square = mm(e_ref[...], e_ref[...])
        e_ref[...] = square
        y_ref[...] = y_ref[...] + mm(y_ref[...], square)

    def residual():
        y = y_ref[...]
        left = ident - y + mm(y, n_ref[...])
        e_ref[...] = left
        return fro2(left)

    size = residual()

    @pl.when(jnp.logical_not(size < 0.25))
    def _():
        system = ident - n_ref[...]
        most = jnp.max(jnp.sum(jnp.abs(system), axis=0, keepdims=True))
        most = most * jnp.max(jnp.sum(jnp.abs(system), axis=1, keepdims=True))
        y_ref[...] = jnp.transpose(system) / most

    size = jnp.where(size < 0.25, size, 1e30)

    def unfinished(state):
        count, now, before = state
        stuck = jnp.logical_and(now < 0.1, now > 0.25 * before)
        return jnp.logical_and(count < 120, jnp.logical_not(jnp.logical_or(before < 1e-6, stuck)))

    def better(state):
        count, now, before = state

        @pl.when(now >= 1e30)
        def _():
            residual()

        y_ref[...] = y_ref[...] + mm(e_ref[...], y_ref[...])
        last = jnp.where(now >= 1e30, 1e30, now)

        def check():
            return residual()

        following = lax.cond(now < 1e-6, lambda: now, check)
        return count + 1, following, last

    lax.while_loop(unfinished, better, (jnp.int32(0), size, F32(1e35)))


def couple_of(spots):
    own = jnp.transpose(spots)
    total = None
    for d in range(3):
        spread = own[:, d : d + 1] - spots[3 + d : 4 + d, :]
        total = spread * spread if total is None else total + spread * spread
    return jnp.exp(-0.5 * total)


def place(core_ref, mine_ref, theirs_ref, full_ref):
    half = mine_ref.shape[0]
    core = core_ref[0]
    full_ref[pl.ds(pl.multiple_of(core * half, half), half), :] = mine_ref[...]
    full_ref[pl.ds(pl.multiple_of((1 - core) * half, half), half), :] = theirs_ref[...]


def spots_of(full_ref, at):
    rank = full_ref.shape[0]
    total = full_ref[0:8, at : at + rank]
    for q in range(1, rank // 8):
        total = total + full_ref[q * 8 : q * 8 + 8, at : at + rank]
    return total


def level_kernel(at, core_ref, mine_ref, theirs_ref, own_ref, other_ref, ans_ref, next_ref, full, n, y, e):
    rank = full.shape[0]
    gram_at, upper_at, upper, gram_o_at, spot_at = at
    place(core_ref, mine_ref, theirs_ref, full)
    couple = couple_of(spots_of(full, spot_at))
    couple_t = jnp.transpose(couple)
    gram = full[:, gram_at : gram_at + rank]
    gram_o = full[:, gram_o_at : gram_o_at + rank]
    far = mm(gram_o, couple_t)
    n[...] = mm(mm(gram, couple), far)
    inverse_into(n, y, e)
    target = mm(other_ref[...], couple_t) - mm(mm(own_ref[:, :rank], couple), far)
    ans = mm(target, y[...])
    ans_ref[...] = ans
    next_ref[...] = own_ref[:, rank : rank + upper] - mm(ans, full[:, upper_at : upper_at + upper])


def call_level(core, mine, theirs, own, other, at):
    rank = 2 * mine.shape[0]
    rows, upper = own.shape[0], at[2]
    vm = pl.BlockSpec(memory_space=pltpu.VMEM)
    return pl.pallas_call(
        functools.partial(level_kernel, at),
        out_shape=(
            jax.ShapeDtypeStruct((rows, rank), F32),
            jax.ShapeDtypeStruct((rows, upper), F32),
        ),
        in_specs=[pl.BlockSpec(memory_space=pltpu.SMEM), vm, vm, vm, vm],
        out_specs=(vm, vm),
        scratch_shapes=[pltpu.VMEM((rank, mine.shape[1]), F32)] + [pltpu.VMEM((rank, rank), F32)] * 3,
        cost_estimate=pl.CostEstimate(flops=16 * 2 * rank**3, bytes_accessed=4 * rank * mine.shape[1], transcendentals=rank * rank),
        compiler_params=pltpu.CompilerParams(vmem_limit_bytes=16 * 1024 * 1024),
    )(core, mine, theirs, own, other)


def top_kernel(core_ref, mine_ref, theirs_ref, low_ref, low2_ref, out_ref, full, low, n, y, e):
    rank = full.shape[0]
    place(core_ref, mine_ref, theirs_ref, full)
    place(core_ref, low_ref, low2_ref, low)
    part = lambda ref, k: ref[:, k * rank : (k + 1) * rank]
    couple = couple_of(spots_of(full, 4 * rank))
    couple_t = jnp.transpose(couple)
    far = mm(part(full, 2), couple_t)
    n[...] = mm(mm(part(full, 0), couple), far)
    inverse_into(n, y, e)
    target = mm(part(full, 3), couple_t) - mm(mm(part(full, 1), couple), far)
    top = mm(target, y[...])
    mid = part(full, 6) - mm(top, part(full, 5))
    bottom = part(low, 2) - mm(top, part(low, 1)) - mm(mid, part(low, 0))
    out_ref[:, 0:rank] = top
    out_ref[:, rank : 2 * rank] = mid
    out_ref[:, 2 * rank : 3 * rank] = bottom


def call_top(core, mine, theirs, low, low2):
    rank = 2 * mine.shape[0]
    vm = pl.BlockSpec(memory_space=pltpu.VMEM)
    return pl.pallas_call(
        top_kernel,
        out_shape=jax.ShapeDtypeStruct((rank, 3 * rank), F32),
        in_specs=[pl.BlockSpec(memory_space=pltpu.SMEM), vm, vm, vm, vm],
        out_specs=vm,
        scratch_shapes=[pltpu.VMEM((rank, mine.shape[1]), F32), pltpu.VMEM((rank, 3 * rank), F32)]
        + [pltpu.VMEM((rank, rank), F32)] * 3,
        cost_estimate=pl.CostEstimate(flops=20 * 2 * rank**3, bytes_accessed=4 * rank * mine.shape[1], transcendentals=rank * rank),
        compiler_params=pltpu.CompilerParams(vmem_limit_bytes=16 * 1024 * 1024),
    )(core, mine, theirs, low, low2)


def swap(value, mask):
    count = lax.axis_size("leaf")
    return lax.ppermute(value, "leaf", [(i, i ^ mask) for i in range(count)])


def spread_to_all(piece):
    copies = jnp.broadcast_to(piece, (lax.axis_size("pts"), *piece.shape))
    got = lax.all_to_all(copies, "pts", 0, 0, tiled=True)
    return got.reshape(-1, piece.shape[-1])


def product_t(columns, panels):
    dots = [
        lax.dot_general(columns, p, (((0,), (0,)), ((), ())), precision=HIGH, preferred_element_type=F32)
        for p in panels
    ]
    return jnp.concatenate(dots, axis=1)


def halves(value, core):
    half = value.shape[-2] // 2
    keep = lax.dynamic_slice_in_dim(value, core * half, half, value.ndim - 2)
    send = lax.dynamic_slice_in_dim(value, (1 - core) * half, half, value.ndim - 2)
    return keep, send


def per_device(
    leaf_solved,
    points,
    panel_top,
    panel_mid,
    panel_low,
    solved_top,
    solved_mid,
    solved_low,
    skeleton_top,
    skeleton_mid,
    skeleton_low,
):
    rows, rank = panel_top.shape
    many = lax.axis_size("pts")
    leaf = lax.axis_index("leaf")
    core, plane = leaf % 2, leaf // 2
    device = leaf * many + lax.axis_index("pts")
    core_arg = core.astype(jnp.int32).reshape(1)
    panels = (panel_low, panel_mid, panel_top)

    take = lambda table, k: lax.dynamic_index_in_dim(table, k, 0, keepdims=False)
    listed = jnp.concatenate(
        [take(skeleton_low, plane), take(skeleton_mid, plane // 2), take(skeleton_top, plane // 4)]
    )
    offsets = listed - device * rows
    select = (offsets[:, None] == jnp.arange(rows, dtype=jnp.int32)[None, :]).astype(F32)
    picked = jnp.einsum("cr,sr->cs", points, select, precision=BEST)
    zero2 = jnp.zeros((2, rank), F32)
    pick_low, pick_mid, pick_top = (picked[:, k * rank : (k + 1) * rank] for k in range(3))

    keep, send = halves(product_t(solved_low, panels), core)
    part = keep + swap(send, 1)
    first = lax.all_to_all(part.reshape(many, -1, 3 * rank), "pts", 0, 0, tiled=True).sum(axis=0)

    bulk = jnp.stack([product_t(c, panels) for c in (solved_mid, solved_top, leaf_solved)])
    keep, send = halves(bulk, core)
    part = (keep + swap(send, 1)).reshape(3, many, -1, 3 * rank)
    rest = lax.all_to_all(part, "pts", 1, 1, tiled=True).sum(axis=1)
    each = rest.shape[1]
    rest = rest.reshape(3 * each, 3 * rank)
    rest_o = swap(rest[:, :rank], 2)

    packed = jnp.concatenate([first[:, :rank], jnp.concatenate([pick_low, jnp.zeros((5, rank), F32)], 0)], 1)
    packed_o = swap(packed, 2)
    spots = jnp.concatenate([pick_low, packed_o[:3, rank:], zero2], 0)
    mine = spread_to_all(jnp.concatenate([first, packed_o[:, :rank], spots], 1))
    theirs = swap(mine, 1)
    low, mid = call_level(core_arg, mine, theirs, rest, rest_o, (0, rank, 2 * rank, 3 * rank, 4 * rank))

    marks = jnp.concatenate([pick_mid, pick_top, zero2], 0)
    mid = jnp.concatenate([mid, jnp.concatenate([marks, jnp.zeros_like(marks)], 1)], 0)
    mid = mid + swap(mid, 2)
    mid_o = swap(mid[:, :rank], 4)
    marks = mid[3 * each :, :rank]
    spots = jnp.concatenate([marks[:3], mid_o[3 * each : 3 * each + 3], zero2], 0)
    mine = spread_to_all(jnp.concatenate([mid[:each], mid_o[:each], spots], 1))
    theirs = swap(mine, 1)
    mine_low = spread_to_all(jnp.concatenate([low[:each], low[each : 2 * each], low[2 * each :]], 1))
    theirs_low = swap(mine_low, 1)
    ans, top = call_level(
        core_arg, mine, theirs, mid[each : 3 * each], mid_o[each : 3 * each], (0, rank, rank, 2 * rank, 3 * rank)
    )

    top = jnp.concatenate([top, marks], 0)
    top = top + swap(top, 4)
    top_o = swap(top, 12)
    spots = jnp.concatenate([top[2 * each + 3 : 2 * each + 6], top_o[2 * each + 3 : 2 * each + 6], zero2], 0)
    mine = spread_to_all(
        jnp.concatenate(
            [top[:each], top[each : 2 * each], top_o[:each], top_o[each : 2 * each], spots, ans[:each], ans[each:]], 1
        )
    )
    theirs = swap(mine, 1)
    answer = call_top(core_arg, mine, theirs, mine_low, theirs_low)
    out = leaf_solved
    for k, columns in enumerate((solved_top, solved_mid, solved_low)):
        out = out - lax.dot_general(
            columns,
            answer[:, k * rank : (k + 1) * rank],
            (((1,), (1,)), ((), ())),
            precision=HIGH,
            preferred_element_type=F32,
        )
    return out


def solution(mesh):
    split = P(("leaf", "pts"), None)
    in_specs = (split, P(None, ("leaf", "pts")), *[split] * 6, P(), P(), P())
    return jax.shard_map(per_device, mesh=mesh, in_specs=in_specs, out_specs=split, check_vma=False)
```

```python
import functools

import jax
import jax.numpy as jnp
from jax import lax
from jax.experimental import pallas as pl
from jax.experimental.pallas import tpu as pltpu
from jax.sharding import PartitionSpec as P


F32 = jnp.float32
BEST = lax.Precision.HIGHEST


def dot(a, b):
    return jnp.dot(a, b, preferred_element_type=F32)


def dot_t(a, b):
    return lax.dot_general(a, b, (((1,), (1,)), ((), ())), preferred_element_type=F32)


def cut(value):
    big = value.astype(jnp.bfloat16)
    return big, (value - big.astype(F32)).astype(jnp.bfloat16)


def mm3(a, b, by=dot):
    (a1, a2), (b1, b2) = a, b
    return by(a1, b1) + (by(a1, b2) + by(a2, b1))


def product_kernel(count, core_ref, *refs):
    sources = refs[: count + 3]
    keep_ref, send_ref, acc, side1, side2, piece1, piece2, come = refs[count + 3 : count + 11]
    held = refs[count + 11 :]
    rows, rank = held[0].shape
    chunk = rank
    loads = []
    for i in range(rows // chunk):
        at = slice(i * chunk, (i + 1) * chunk)
        for k, (source, place_) in enumerate(zip(sources, held)):
            load = pltpu.make_async_copy(source.at[at, :], place_.at[at, :], come.at[i, k])
            load.start()
            loads.append(load)
    for i in range(rows // chunk):
        at = slice(i * chunk, (i + 1) * chunk)
        for load in loads[i * (count + 3) : (i + 1) * (count + 3)]:
            load.wait()
        for b in range(count):
            band = slice(b * rank, (b + 1) * rank)
            side1[band, at], side2[band, at] = cut(jnp.transpose(held[b][at, :]))
        for k in range(3):
            band = slice(k * rank, (k + 1) * rank)
            piece1[at, band], piece2[at, band] = cut(held[count + k][at, :])
    for k in range(3):
        band = slice(k * rank, (k + 1) * rank)
        one, two = piece1[:, band], piece2[:, band]
        acc[:, band] = dot(side1[...], one) + (dot(side1[...], two) + dot(side2[...], one))
    core = core_ref[0]
    for ref, which in ((keep_ref, core), (send_ref, 1 - core)):
        for p in range(keep_ref.shape[0]):
            for b in range(count):
                row = pl.multiple_of(b * rank + which * (rank // 2) + p * 8, 8)
                ref[p, :, b * 3 * rank : (b + 1) * 3 * rank] = acc[pl.ds(row, 8), :]


def call_product(core, columns, panels, many):
    rows, rank = panels[0].shape
    count = len(columns)
    half = jax.ShapeDtypeStruct((many, 8, count * 3 * rank), F32)
    vm = pl.BlockSpec(memory_space=pltpu.VMEM)
    return pl.pallas_call(
        functools.partial(product_kernel, count),
        out_shape=(half, half),
        in_specs=[pl.BlockSpec(memory_space=pltpu.SMEM)] + [pl.BlockSpec(memory_space=pltpu.HBM)] * (count + 3),
        out_specs=(vm, vm),
        scratch_shapes=[pltpu.VMEM((count * rank, 3 * rank), F32)]
        + [pltpu.VMEM((count * rank, rows), jnp.bfloat16)] * 2
        + [pltpu.VMEM((rows, 3 * rank), jnp.bfloat16)] * 2
        + [pltpu.SemaphoreType.DMA((rows // rank, count + 3))]
        + [pltpu.VMEM((rows, rank), F32)] * (count + 3),
        cost_estimate=pl.CostEstimate(
            flops=count * 18 * rows * rank * rank, bytes_accessed=4 * rows * rank * (count + 3), transcendentals=0
        ),
        compiler_params=pltpu.CompilerParams(vmem_limit_bytes=60 * 1024 * 1024),
    )(core, *columns, *panels)


def fro2(value):
    return jnp.sum(value * value)


def inverse_into(n_ref, y_ref, e_ref):
    rank = n_ref.shape[0]
    row = lax.broadcasted_iota(jnp.int32, (rank, rank), 0)
    col = lax.broadcasted_iota(jnp.int32, (rank, rank), 1)
    ident = jnp.where(row == col, 1.0, 0.0).astype(F32)
    y_ref[...] = ident + n_ref[...]
    e_ref[...] = n_ref[...]

    @pl.loop(0, 2)
    def _(step):
        before = cut(e_ref[...])
        square = mm3(before, before)
        e_ref[...] = square
        y = y_ref[...]
        y_ref[...] = y + mm3(cut(y), cut(square))

    def residual():
        y = y_ref[...]
        left = ident - y + mm3(cut(y), cut(n_ref[...]))
        e_ref[...] = left
        return fro2(left)

    def improve():
        y = y_ref[...]
        y_ref[...] = y + mm3(cut(e_ref[...]), cut(y))

    size = residual()
    good = size < 0.25

    @pl.when(jnp.logical_not(good))
    def _():
        system = ident - n_ref[...]
        most = jnp.max(jnp.sum(jnp.abs(system), axis=0, keepdims=True))
        most = most * jnp.max(jnp.sum(jnp.abs(system), axis=1, keepdims=True))
        y_ref[...] = jnp.transpose(system) / most
        residual()

    def unfinished(state):
        count, now, before = state
        stuck = jnp.logical_and(now < 0.1, now > 0.25 * before)
        return jnp.logical_and(count < 120, jnp.logical_not(jnp.logical_or(now < 4e-6, stuck)))

    def better(state):
        count, now, _ = state
        improve()
        return count + 1, residual(), now

    lax.while_loop(unfinished, better, (jnp.int32(0), jnp.where(good, size, F32(1e30)), F32(1e35)))
    improve()


def couple_of(spots):
    own = jnp.transpose(spots)
    total = None
    for d in range(3):
        spread = own[:, d : d + 1] - spots[3 + d : 4 + d, :]
        total = spread * spread if total is None else total + spread * spread
    return jnp.exp(-0.5 * total)


def place(core_ref, mine_ref, theirs_ref, full_ref):
    half = mine_ref.shape[0]
    core = core_ref[0]
    full_ref[pl.ds(pl.multiple_of(core * half, half), half), :] = mine_ref[...]
    full_ref[pl.ds(pl.multiple_of((1 - core) * half, half), half), :] = theirs_ref[...]


def spots_of(mine_ref, theirs_ref, at):
    rank = 2 * mine_ref.shape[0]
    total = None
    for ref in (mine_ref, theirs_ref):
        for q in range(rank // 16):
            some = ref[q * 8 : q * 8 + 8, at : at + rank]
            total = some if total is None else total + some
    return total


def level_kernel(at, core_ref, mine_ref, theirs_ref, own_ref, other_ref, ans_ref, next_ref, full, n, y, e):
    rank = full.shape[0]
    gram_at, upper_at, upper, gram_o_at, spot_at = at
    place(core_ref, mine_ref, theirs_ref, full)
    couple = couple_of(spots_of(mine_ref, theirs_ref, spot_at))
    couple_t = jnp.transpose(couple)
    gram = full[:, gram_at : gram_at + rank]
    gram_o = full[:, gram_o_at : gram_o_at + rank]
    c, c_t = cut(couple), cut(couple_t)
    far = cut(mm3(cut(gram_o), c_t))
    n[...] = mm3(cut(mm3(cut(gram), c)), far)
    inverse_into(n, y, e)
    target = mm3(cut(other_ref[...]), c_t) - mm3(cut(mm3(cut(own_ref[:, :rank]), c)), far)
    ans = mm3(cut(target), cut(y[...]))
    ans_ref[...] = ans
    next_ref[...] = own_ref[:, rank : rank + upper] - mm3(cut(ans), cut(full[:, upper_at : upper_at + upper]))


def call_level(core, mine, theirs, own, other, at):
    rank = 2 * mine.shape[0]
    rows, upper = own.shape[0], at[2]
    vm = pl.BlockSpec(memory_space=pltpu.VMEM)
    return pl.pallas_call(
        functools.partial(level_kernel, at),
        out_shape=(
            jax.ShapeDtypeStruct((rows, rank), F32),
            jax.ShapeDtypeStruct((rows, upper), F32),
        ),
        in_specs=[pl.BlockSpec(memory_space=pltpu.SMEM), vm, vm, vm, vm],
        out_specs=(vm, vm),
        scratch_shapes=[pltpu.VMEM((rank, mine.shape[1]), F32)] + [pltpu.VMEM((rank, rank), F32)] * 3,
        cost_estimate=pl.CostEstimate(
            flops=80 * 2 * rank**3, bytes_accessed=4 * rank * mine.shape[1], transcendentals=rank * rank
        ),
        compiler_params=pltpu.CompilerParams(vmem_limit_bytes=16 * 1024 * 1024),
    )(core, mine, theirs, own, other)


def top_kernel(core_ref, mine_ref, theirs_ref, *refs):
    held, out_ref = refs[:4], refs[4]
    full, n, y, e, stacked, result, go = refs[5:]
    rank = full.shape[0]
    place(core_ref, mine_ref, theirs_ref, full)
    part = lambda k: full[:, k * rank : (k + 1) * rank]
    couple = couple_of(spots_of(mine_ref, theirs_ref, 4 * rank))
    couple_t = jnp.transpose(couple)
    c, c_t = cut(couple), cut(couple_t)
    far = cut(mm3(cut(part(2)), c_t))
    n[...] = mm3(cut(mm3(cut(part(0)), c)), far)
    inverse_into(n, y, e)
    target = mm3(cut(part(3)), c_t) - mm3(cut(mm3(cut(part(1)), c)), far)
    top = cut(mm3(cut(target), cut(y[...])))
    mid = cut(part(6) - mm3(top, cut(part(5))))
    low = cut(part(9) - mm3(top, cut(part(8))) - mm3(mid, cut(part(7))))
    for k, (one, two) in enumerate((top, mid, low)):
        stacked[0, :, k * rank : (k + 1) * rank] = one
        stacked[1, :, k * rank : (k + 1) * rank] = two
    rows = result.shape[0]
    chunk = rows // 4
    stores = []
    for i in range(4):
        at = slice(i * chunk, (i + 1) * chunk)
        total = held[0][at, :]
        for k in range(3):
            lanes = slice(k * rank, (k + 1) * rank)
            total = total - mm3(cut(held[1 + k][at, :]), (stacked[0, :, lanes], stacked[1, :, lanes]), dot_t)
        result[at, :] = total
        store = pltpu.make_async_copy(result.at[at, :], out_ref.at[at, :], go.at[i])
        store.start()
        stores.append(store)
    for store in stores:
        store.wait()


def call_top(core, mine, theirs, carry):
    rank = 2 * mine.shape[0]
    rows = carry[0].shape[0]
    vm = pl.BlockSpec(memory_space=pltpu.VMEM)
    far = pl.BlockSpec(memory_space=pltpu.HBM)
    return pl.pallas_call(
        top_kernel,
        out_shape=jax.ShapeDtypeStruct((rows, rank), F32),
        in_specs=[pl.BlockSpec(memory_space=pltpu.SMEM), vm] * 1 + [vm] * 5,
        out_specs=far,
        scratch_shapes=[pltpu.VMEM((rank, mine.shape[1]), F32)]
        + [pltpu.VMEM((rank, rank), F32)] * 3
        + [pltpu.VMEM((2, rank, 3 * rank), jnp.bfloat16), pltpu.VMEM((rows, rank), F32)]
        + [pltpu.SemaphoreType.DMA((4,))],
        cost_estimate=pl.CostEstimate(
            flops=100 * 2 * rank**3, bytes_accessed=4 * rank * mine.shape[1] + 20 * rows * rank, transcendentals=rank * rank
        ),
        compiler_params=pltpu.CompilerParams(vmem_limit_bytes=32 * 1024 * 1024),
    )(core, mine, theirs, *carry)


def swap(value, mask):
    count = lax.axis_size("leaf")
    return lax.ppermute(value, "leaf", [(i, i ^ mask) for i in range(count)])


def to_all(piece):
    return jnp.broadcast_to(piece, (lax.axis_size("pts"), *piece.shape))


def exchanged(pieces):
    return lax.all_to_all(pieces, "pts", 0, 0, tiled=True)


def spread_to_all(piece):
    return exchanged(to_all(piece)).reshape(-1, piece.shape[-1])


def per_device(
    leaf_solved,
    points,
    panel_top,
    panel_mid,
    panel_low,
    solved_top,
    solved_mid,
    solved_low,
    skeleton_top,
    skeleton_mid,
    skeleton_low,
):
    rows, rank = panel_top.shape
    many = lax.axis_size("pts")
    leaf = lax.axis_index("leaf")
    core, plane = leaf % 2, leaf // 2
    device = leaf * many + lax.axis_index("pts")
    core_arg = core.astype(jnp.int32).reshape(1)
    panels = (panel_low, panel_mid, panel_top)
    zero2 = jnp.zeros((2, rank), F32)
    each = rank // (2 * many)

    keep, send = call_product(core_arg, (solved_low,), panels, many)
    first = exchanged(keep + swap(send, 1)).sum(axis=0)
    keep, send = call_product(core_arg, (solved_mid, solved_top, leaf_solved), panels, many)
    rest = keep + swap(send, 1)
    take = lambda table, k: lax.dynamic_index_in_dim(table, k, 0, keepdims=False)
    listed = jnp.concatenate(
        [take(skeleton_low, plane), take(skeleton_mid, plane // 2), take(skeleton_top, plane // 4)]
    )
    offsets = listed - device * rows
    select = (offsets[:, None] == jnp.arange(rows, dtype=jnp.int32)[None, :]).astype(F32)
    picked = jnp.einsum("cr,sr->cs", points, select, precision=BEST)
    pick_low, pick_mid, pick_top = (picked[:, k * rank : (k + 1) * rank] for k in range(3))

    mark = jnp.concatenate([pick_low, jnp.zeros((5, rank), F32)], 0)
    first_o = swap(jnp.concatenate([first[:, :rank], mark], 1), 2)
    spots = jnp.concatenate([pick_low, first_o[:3, rank:], zero2], 0)
    piece = jnp.concatenate([first, first_o[:, :rank], spots], 1)
    wide = piece.shape[1]
    got = exchanged(jnp.concatenate([to_all(piece), rest], 2))
    mine = got[:, :, :wide].reshape(-1, wide)
    theirs = swap(mine, 1)
    rest = got[:, :, wide:].sum(axis=0)
    own = jnp.concatenate([rest[:, 3 * k * rank : 3 * (k + 1) * rank] for k in range(3)], 0)
    other = swap(own[:, :rank], 2)
    low, mid = call_level(core_arg, mine, theirs, own, other, (0, rank, 2 * rank, 3 * rank, 4 * rank))

    marks = jnp.concatenate([pick_mid, pick_top, zero2], 0)
    mid = jnp.concatenate([mid, jnp.concatenate([marks, jnp.zeros_like(marks)], 1)], 0)
    mid = mid + swap(mid, 2)
    mid_o = swap(mid[:, :rank], 4)
    marks, marks_o = mid[3 * each :, :rank], mid_o[3 * each :]
    spots = jnp.concatenate([marks[:3], marks_o[:3], zero2], 0)
    marks = marks + marks_o
    mine = spread_to_all(jnp.concatenate([mid[:each], mid_o[:each], spots], 1))
    theirs = swap(mine, 1)
    ans, top = call_level(
        core_arg, mine, theirs, mid[each : 3 * each], mid_o[each : 3 * each], (0, rank, rank, 2 * rank, 3 * rank)
    )

    top = top + swap(top, 4)
    top_o = swap(jnp.concatenate([top, marks], 0), 8)
    spots = jnp.concatenate([marks[3:6], top_o[2 * each + 3 : 2 * each + 6], zero2], 0)
    blocks = [top[:each], top[each:], top_o[:each], top_o[each : 2 * each], spots]
    blocks += [ans[:each], ans[each:], low[:each], low[each : 2 * each], low[2 * each :]]
    mine = spread_to_all(jnp.concatenate(blocks, 1))
    theirs = swap(mine, 1)
    return call_top(core_arg, mine, theirs, (leaf_solved, solved_top, solved_mid, solved_low))


def solution(mesh):
    split = P(("leaf", "pts"), None)
    in_specs = (split, P(None, ("leaf", "pts")), *[split] * 6, P(), P(), P())

    return jax.shard_map(per_device, mesh=mesh, in_specs=in_specs, out_specs=split, check_vma=False)
```

```python
import functools

import jax
import jax.numpy as jnp
from jax import lax
from jax.experimental import pallas as pl
from jax.experimental.pallas import tpu as pltpu
from jax.sharding import PartitionSpec as P


F32 = jnp.float32
BEST = lax.Precision.HIGHEST


def dot(a, b):
    return jnp.dot(a, b, preferred_element_type=F32)


def dot_t(a, b):
    return lax.dot_general(a, b, (((1,), (1,)), ((), ())), preferred_element_type=F32)


def cut(value):
    big = value.astype(jnp.bfloat16)
    return big, (value - big.astype(F32)).astype(jnp.bfloat16)


def mm3(a, b, by=dot):
    (a1, a2), (b1, b2) = a, b
    rows = a1.shape[0]
    if rows % 128:
        return by(a1, b1) + (by(a1, b2) + by(a2, b1))
    both = by(jnp.concatenate([a1, a2], 0), b1)
    return both[:rows] + (both[rows:] + by(a1, b2))


def product_kernel(count, core_ref, *refs):
    sources = refs[: count + 3]
    keep_ref, send_ref, acc, come = refs[count + 3 : count + 7]
    held = refs[count + 7 :]
    rows, rank = held[0].shape
    chunk = rank
    loads = []
    for i in range(rows // chunk):
        at = slice(i * chunk, (i + 1) * chunk)
        for k, (source, place_) in enumerate(zip(sources, held)):
            load = pltpu.make_async_copy(source.at[at, :], place_.at[at, :], come.at[i, k])
            load.start()
            loads.append(load)
    for i in range(rows // chunk):
        at = slice(i * chunk, (i + 1) * chunk)
        for load in loads[i * (count + 3) : (i + 1) * (count + 3)]:
            load.wait()
        sides = [cut(jnp.transpose(held[b][at, :])) for b in range(count)]
        side = tuple(jnp.concatenate(part, 0) for part in zip(*sides))
        for k in range(3):
            band = slice(k * rank, (k + 1) * rank)
            term = mm3(side, cut(held[count + k][at, :]))
            acc[:, band] = term if i == 0 else acc[:, band] + term
    core = core_ref[0]
    for ref, which in ((keep_ref, core), (send_ref, 1 - core)):
        for p in range(keep_ref.shape[0]):
            for b in range(count):
                row = pl.multiple_of(b * rank + which * (rank // 2) + p * 8, 8)
                ref[p, :, b * 3 * rank : (b + 1) * 3 * rank] = acc[pl.ds(row, 8), :]


def call_product(core, columns, panels, many):
    rows, rank = panels[0].shape
    count = len(columns)
    half = jax.ShapeDtypeStruct((many, 8, count * 3 * rank), F32)
    vm = pl.BlockSpec(memory_space=pltpu.VMEM)
    return pl.pallas_call(
        functools.partial(product_kernel, count),
        out_shape=(half, half),
        in_specs=[pl.BlockSpec(memory_space=pltpu.SMEM)] + [pl.BlockSpec(memory_space=pltpu.HBM)] * (count + 3),
        out_specs=(vm, vm),
        scratch_shapes=[pltpu.VMEM((count * rank, 3 * rank), F32)]
        + [pltpu.SemaphoreType.DMA((rows // rank, count + 3))]
        + [pltpu.VMEM((rows, rank), F32)] * (count + 3),
        cost_estimate=pl.CostEstimate(
            flops=count * 18 * rows * rank * rank, bytes_accessed=4 * rows * rank * (count + 3), transcendentals=0
        ),
        compiler_params=pltpu.CompilerParams(vmem_limit_bytes=52 * 1024 * 1024),
    )(core, *columns, *panels)


def fro2(value):
    return jnp.sum(value * value)


def inverse_into(n_ref, y_ref, e_ref):
    rank = n_ref.shape[0]
    row = lax.broadcasted_iota(jnp.int32, (rank, rank), 0)
    col = lax.broadcasted_iota(jnp.int32, (rank, rank), 1)
    ident = jnp.where(row == col, 1.0, 0.0).astype(F32)
    y_ref[...] = ident + n_ref[...]
    e_ref[...] = n_ref[...]

    for _ in range(2):
        some = e_ref[...].astype(jnp.bfloat16)
        square = dot(some, some)
        e_ref[...] = square
        y = y_ref[...]
        y_ref[...] = y + dot(y.astype(jnp.bfloat16), square.astype(jnp.bfloat16))

    def residual():
        y = y_ref[...]
        left = ident - y + mm3(cut(y), cut(n_ref[...]))
        e_ref[...] = left
        return fro2(left)

    def improve():
        y = y_ref[...]
        y_ref[...] = y + mm3(cut(e_ref[...]), cut(y))

    size = residual()
    good = size < 0.25

    @pl.when(jnp.logical_not(good))
    def _():
        system = ident - n_ref[...]
        most = jnp.max(jnp.sum(jnp.abs(system), axis=0, keepdims=True))
        most = most * jnp.max(jnp.sum(jnp.abs(system), axis=1, keepdims=True))
        y_ref[...] = jnp.transpose(system) / most
        residual()

    def unfinished(state):
        count, now, before = state
        stuck = jnp.logical_and(now < 0.1, now > 0.25 * before)
        return jnp.logical_and(count < 120, jnp.logical_not(jnp.logical_or(now < 4e-6, stuck)))

    def better(state):
        count, now, _ = state
        improve()
        return count + 1, residual(), now

    lax.while_loop(unfinished, better, (jnp.int32(0), jnp.where(good, size, F32(1e30)), F32(1e35)))
    improve()


def couple_of(spots):
    own = jnp.transpose(spots)
    total = None
    for d in range(3):
        spread = own[:, d : d + 1] - spots[3 + d : 4 + d, :]
        total = spread * spread if total is None else total + spread * spread
    return jnp.exp(-0.5 * total)


def place(core_ref, mine_ref, theirs_ref, full_ref):
    half = mine_ref.shape[0]
    core = core_ref[0]
    full_ref[pl.ds(pl.multiple_of(core * half, half), half), :] = mine_ref[...]
    full_ref[pl.ds(pl.multiple_of((1 - core) * half, half), half), :] = theirs_ref[...]


def spots_of(mine_ref, theirs_ref, at):
    rank = 2 * mine_ref.shape[0]
    total = None
    for ref in (mine_ref, theirs_ref):
        for q in range(rank // 16):
            some = ref[q * 8 : q * 8 + 8, at : at + rank]
            total = some if total is None else total + some
    return total


def level_kernel(at, core_ref, mine_ref, theirs_ref, own_ref, other_ref, ans_ref, next_ref, full, n, y, e):
    rank = full.shape[0]
    gram_at, upper_at, upper, gram_o_at, spot_at = at
    place(core_ref, mine_ref, theirs_ref, full)
    couple = couple_of(spots_of(mine_ref, theirs_ref, spot_at))
    couple_t = jnp.transpose(couple)
    gram = full[:, gram_at : gram_at + rank]
    gram_o = full[:, gram_o_at : gram_o_at + rank]
    c, c_t = cut(couple), cut(couple_t)
    far = cut(mm3(cut(gram_o), c_t))
    n[...] = mm3(cut(mm3(cut(gram), c)), far)
    inverse_into(n, y, e)
    target = mm3(cut(other_ref[...]), c_t) - mm3(cut(mm3(cut(own_ref[:, :rank]), c)), far)
    ans = mm3(cut(target), cut(y[...]))
    ans_ref[...] = ans
    next_ref[...] = own_ref[:, rank : rank + upper] - mm3(cut(ans), cut(full[:, upper_at : upper_at + upper]))


def solve_kernel(at, core_ref, mine_ref, theirs_ref, couple_ref, far_ref, y_ref, up_ref, full, n, e):
    rank = full.shape[0]
    gram_at, upper_at, upper, gram_o_at, spot_at = at
    place(core_ref, mine_ref, theirs_ref, full)
    couple = couple_of(spots_of(mine_ref, theirs_ref, spot_at))
    far = mm3(cut(full[:, gram_o_at : gram_o_at + rank]), cut(jnp.transpose(couple)))
    n[...] = mm3(cut(mm3(cut(full[:, gram_at : gram_at + rank]), cut(couple))), cut(far))
    couple_ref[...] = couple
    far_ref[...] = far
    up_ref[...] = full[:, upper_at : upper_at + upper]
    inverse_into(n, y_ref, e)


def call_solve(core, mine, theirs, at):
    rank, upper = 2 * mine.shape[0], at[2]
    vm = pl.BlockSpec(memory_space=pltpu.VMEM)
    square = jax.ShapeDtypeStruct((rank, rank), F32)
    return pl.pallas_call(
        functools.partial(solve_kernel, at),
        out_shape=(square, square, square, jax.ShapeDtypeStruct((rank, upper), F32)),
        in_specs=[pl.BlockSpec(memory_space=pltpu.SMEM), vm, vm],
        out_specs=(vm, vm, vm, vm),
        scratch_shapes=[pltpu.VMEM((rank, mine.shape[1]), F32)] + [pltpu.VMEM((rank, rank), F32)] * 2,
        cost_estimate=pl.CostEstimate(
            flops=60 * 2 * rank**3, bytes_accessed=4 * rank * mine.shape[1], transcendentals=rank * rank
        ),
        compiler_params=pltpu.CompilerParams(vmem_limit_bytes=16 * 1024 * 1024),
    )(core, mine, theirs)


def apply_kernel(couple_ref, far_ref, y_ref, up_ref, own_ref, other_ref, ans_ref, next_ref):
    rank = couple_ref.shape[0]
    couple = couple_ref[...]
    near = mm3(cut(own_ref[:, :rank]), cut(couple))
    target = mm3(cut(other_ref[...]), cut(couple), dot_t) - mm3(cut(near), cut(far_ref[...]))
    ans = mm3(cut(target), cut(y_ref[...]))
    ans_ref[...] = ans
    next_ref[...] = own_ref[:, rank:] - mm3(cut(ans), cut(up_ref[...]))


def call_apply(solved, own, other):
    rank, upper = solved[3].shape
    rows = own.shape[0]
    vm = pl.BlockSpec(memory_space=pltpu.VMEM)
    return pl.pallas_call(
        apply_kernel,
        out_shape=(
            jax.ShapeDtypeStruct((rows, rank), F32),
            jax.ShapeDtypeStruct((rows, upper), F32),
        ),
        in_specs=[vm] * 6,
        out_specs=(vm, vm),
        cost_estimate=pl.CostEstimate(
            flops=30 * 2 * rows * rank**2, bytes_accessed=4 * rank * (3 * rank + upper), transcendentals=0
        ),
        compiler_params=pltpu.CompilerParams(vmem_limit_bytes=16 * 1024 * 1024),
    )(*solved, own, other)


def call_level(core, mine, theirs, own, other, at):
    rank = 2 * mine.shape[0]
    rows, upper = own.shape[0], at[2]
    vm = pl.BlockSpec(memory_space=pltpu.VMEM)
    return pl.pallas_call(
        functools.partial(level_kernel, at),
        out_shape=(
            jax.ShapeDtypeStruct((rows, rank), F32),
            jax.ShapeDtypeStruct((rows, upper), F32),
        ),
        in_specs=[pl.BlockSpec(memory_space=pltpu.SMEM), vm, vm, vm, vm],
        out_specs=(vm, vm),
        scratch_shapes=[pltpu.VMEM((rank, mine.shape[1]), F32)] + [pltpu.VMEM((rank, rank), F32)] * 3,
        cost_estimate=pl.CostEstimate(
            flops=80 * 2 * rank**3, bytes_accessed=4 * rank * mine.shape[1], transcendentals=rank * rank
        ),
        compiler_params=pltpu.CompilerParams(vmem_limit_bytes=16 * 1024 * 1024),
    )(core, mine, theirs, own, other)


def top_kernel(core_ref, mine_ref, theirs_ref, *refs):
    held, out_ref = refs[:4], refs[4]
    full, n, y, e, stacked, result, go = refs[5:]
    rank = full.shape[0]
    place(core_ref, mine_ref, theirs_ref, full)
    part = lambda k: full[:, k * rank : (k + 1) * rank]
    couple = couple_of(spots_of(mine_ref, theirs_ref, 4 * rank))
    couple_t = jnp.transpose(couple)
    c, c_t = cut(couple), cut(couple_t)
    far = cut(mm3(cut(part(2)), c_t))
    n[...] = mm3(cut(mm3(cut(part(0)), c)), far)
    inverse_into(n, y, e)
    target = mm3(cut(part(3)), c_t) - mm3(cut(mm3(cut(part(1)), c)), far)
    top = cut(mm3(cut(target), cut(y[...])))
    mid = cut(part(6) - mm3(top, cut(part(5))))
    low = cut(part(9) - mm3(top, cut(part(8))) - mm3(mid, cut(part(7))))
    for k, (one, two) in enumerate((top, mid, low)):
        stacked[0, :, k * rank : (k + 1) * rank] = one
        stacked[1, :, k * rank : (k + 1) * rank] = two
    rows = result.shape[0]
    chunk = rows // 4
    stores = []
    for i in range(4):
        at = slice(i * chunk, (i + 1) * chunk)
        sides = [cut(held[1 + k][at, :]) for k in range(3)]
        side = tuple(jnp.concatenate(part, 1) for part in zip(*sides))
        total = held[0][at, :] - mm3(side, (stacked[0], stacked[1]), dot_t)
        result[at, :] = total
        store = pltpu.make_async_copy(result.at[at, :], out_ref.at[at, :], go.at[i])
        store.start()
        stores.append(store)
    for store in stores:
        store.wait()


def call_top(core, mine, theirs, carry):
    rank = 2 * mine.shape[0]
    rows = carry[0].shape[0]
    vm = pl.BlockSpec(memory_space=pltpu.VMEM)
    far = pl.BlockSpec(memory_space=pltpu.HBM)
    return pl.pallas_call(
        top_kernel,
        out_shape=jax.ShapeDtypeStruct((rows, rank), F32),
        in_specs=[pl.BlockSpec(memory_space=pltpu.SMEM), vm] * 1 + [vm] * 5,
        out_specs=far,
        scratch_shapes=[pltpu.VMEM((rank, mine.shape[1]), F32)]
        + [pltpu.VMEM((rank, rank), F32)] * 3
        + [pltpu.VMEM((2, rank, 3 * rank), jnp.bfloat16), pltpu.VMEM((rows, rank), F32)]
        + [pltpu.SemaphoreType.DMA((4,))],
        cost_estimate=pl.CostEstimate(
            flops=100 * 2 * rank**3, bytes_accessed=4 * rank * mine.shape[1] + 20 * rows * rank, transcendentals=rank * rank
        ),
        compiler_params=pltpu.CompilerParams(vmem_limit_bytes=32 * 1024 * 1024),
    )(core, mine, theirs, *carry)


def swap(value, mask):
    count = lax.axis_size("leaf")
    return lax.ppermute(value, "leaf", [(i, i ^ mask) for i in range(count)])


def to_all(piece):
    return jnp.broadcast_to(piece, (lax.axis_size("pts"), *piece.shape))


def exchanged(pieces):
    return lax.all_to_all(pieces, "pts", 0, 0, tiled=True)


def spread_to_all(piece):
    return exchanged(to_all(piece)).reshape(-1, piece.shape[-1])


def per_device(
    leaf_solved,
    points,
    panel_top,
    panel_mid,
    panel_low,
    solved_top,
    solved_mid,
    solved_low,
    skeleton_top,
    skeleton_mid,
    skeleton_low,
):
    rows, rank = panel_top.shape
    many = lax.axis_size("pts")
    leaf = lax.axis_index("leaf")
    core, plane = leaf % 2, leaf // 2
    device = leaf * many + lax.axis_index("pts")
    core_arg = core.astype(jnp.int32).reshape(1)
    panels = (panel_low, panel_mid, panel_top)
    zero2 = jnp.zeros((2, rank), F32)
    each = rank // (2 * many)

    keep, send = call_product(core_arg, (solved_low, solved_mid), panels, many)
    both = exchanged(keep + swap(send, 1)).sum(axis=0)
    first, middle = both[:, : 3 * rank], both[:, 3 * rank :]
    keep, send = call_product(core_arg, (solved_top, leaf_solved), panels, many)
    rest = keep + swap(send, 1)
    take = lambda table, k: lax.dynamic_index_in_dim(table, k, 0, keepdims=False)
    listed = jnp.concatenate(
        [take(skeleton_low, plane), take(skeleton_mid, plane // 2), take(skeleton_top, plane // 4)]
    )
    offsets = listed - device * rows
    select = (offsets[:, None] == jnp.arange(rows, dtype=jnp.int32)[None, :]).astype(F32)
    picked = jnp.einsum("cr,sr->cs", points, select, precision=BEST)
    pick_low, pick_mid, pick_top = (picked[:, k * rank : (k + 1) * rank] for k in range(3))

    mark = jnp.concatenate([pick_low, jnp.zeros((5, rank), F32)], 0)
    first_o = swap(jnp.concatenate([first[:, :rank], mark], 1), 2)
    spots = jnp.concatenate([pick_low, first_o[:3, rank:], zero2], 0)
    piece = jnp.concatenate([first, first_o[:, :rank], spots], 1)
    wide = piece.shape[1]
    got = exchanged(jnp.concatenate([to_all(piece), rest], 2))
    mine = got[:, :, :wide].reshape(-1, wide)
    theirs = swap(mine, 1)
    rest = got[:, :, wide:].sum(axis=0)
    own = jnp.concatenate([middle, rest[:, : 3 * rank], rest[:, 3 * rank :]], 0)
    other = swap(own[:, :rank], 2)
    solved = call_solve(core_arg, mine, theirs, (0, rank, 2 * rank, 3 * rank, 4 * rank))
    low, mid = call_apply(solved, own, other)

    marks = jnp.concatenate([pick_mid, pick_top, zero2], 0)
    mid = jnp.concatenate([mid, jnp.concatenate([marks, jnp.zeros_like(marks)], 1)], 0)
    mid = mid + swap(mid, 2)
    mid_o = swap(mid[:, :rank], 4)
    marks, marks_o = mid[3 * each :, :rank], mid_o[3 * each :]
    spots = jnp.concatenate([marks[:3], marks_o[:3], zero2], 0)
    marks = marks + marks_o
    mine = spread_to_all(jnp.concatenate([mid[:each], mid_o[:each], spots], 1))
    theirs = swap(mine, 1)
    ans, top = call_level(
        core_arg, mine, theirs, mid[each : 3 * each], mid_o[each : 3 * each], (0, rank, rank, 2 * rank, 3 * rank)
    )

    far1, far2 = swap(jnp.concatenate([top, marks], 0), 8), swap(top, 12)
    top, top_o = top + swap(top, 4), far1[: 2 * each] + far2
    spots = jnp.concatenate([marks[3:6], far1[2 * each + 3 : 2 * each + 6], zero2], 0)
    blocks = [top[:each], top[each:], top_o[:each], top_o[each:], spots]
    blocks += [ans[:each], ans[each:], low[:each], low[each : 2 * each], low[2 * each :]]
    mine = spread_to_all(jnp.concatenate(blocks, 1))
    theirs = swap(mine, 1)
    return call_top(core_arg, mine, theirs, (leaf_solved, solved_top, solved_mid, solved_low))


def solution(mesh):
    split = P(("leaf", "pts"), None)
    in_specs = (split, P(None, ("leaf", "pts")), *[split] * 6, P(), P(), P())

    return jax.shard_map(per_device, mesh=mesh, in_specs=in_specs, out_specs=split, check_vma=False)
```

```python
import functools

import jax
import jax.numpy as jnp
from jax import lax
from jax.experimental import pallas as pl
from jax.experimental.pallas import tpu as pltpu
from jax.sharding import PartitionSpec as P


F32 = jnp.float32
BEST = lax.Precision.HIGHEST


def dot(a, b):
    return jnp.dot(a, b, preferred_element_type=F32)


def dot_t(a, b):
    return lax.dot_general(a, b, (((1,), (1,)), ((), ())), preferred_element_type=F32)


def cut(value):
    big = value.astype(jnp.bfloat16)
    return big, (value - big.astype(F32)).astype(jnp.bfloat16)


def mm3(a, b, by=dot):
    (a1, a2), (b1, b2) = a, b
    rows = a1.shape[0]
    if rows % 128:
        return by(a1, b1) + (by(a1, b2) + by(a2, b1))
    both = by(jnp.concatenate([a1, a2], 0), b1)
    return both[:rows] + (both[rows:] + by(a1, b2))


def product_kernel(count, core_ref, *refs):
    sources = refs[: count + 3]
    keep_ref, send_ref, acc, come = refs[count + 3 : count + 7]
    held = refs[count + 7 :]
    rows, rank = held[0].shape
    chunk = rank
    loads = []
    for i in range(rows // chunk):
        at = slice(i * chunk, (i + 1) * chunk)
        for k, (source, place_) in enumerate(zip(sources, held)):
            load = pltpu.make_async_copy(source.at[at, :], place_.at[at, :], come.at[i, k])
            load.start()
            loads.append(load)
    for i in range(rows // chunk):
        at = slice(i * chunk, (i + 1) * chunk)
        for load in loads[i * (count + 3) : (i + 1) * (count + 3)]:
            load.wait()
        sides = [cut(jnp.transpose(held[b][at, :])) for b in range(count)]
        side = tuple(jnp.concatenate(part, 0) for part in zip(*sides))
        for k in range(3):
            band = slice(k * rank, (k + 1) * rank)
            term = mm3(side, cut(held[count + k][at, :]))
            acc[:, band] = term if i == 0 else acc[:, band] + term
    core = core_ref[0]
    for ref, which in ((keep_ref, core), (send_ref, 1 - core)):
        for p in range(keep_ref.shape[0]):
            for b in range(count):
                row = pl.multiple_of(b * rank + which * (rank // 2) + p * 8, 8)
                ref[p, :, b * 3 * rank : (b + 1) * 3 * rank] = acc[pl.ds(row, 8), :]


def call_product(core, columns, panels, many):
    rows, rank = panels[0].shape
    count = len(columns)
    half = jax.ShapeDtypeStruct((many, 8, count * 3 * rank), F32)
    vm = pl.BlockSpec(memory_space=pltpu.VMEM)
    return pl.pallas_call(
        functools.partial(product_kernel, count),
        out_shape=(half, half),
        in_specs=[pl.BlockSpec(memory_space=pltpu.SMEM)] + [pl.BlockSpec(memory_space=pltpu.HBM)] * (count + 3),
        out_specs=(vm, vm),
        scratch_shapes=[pltpu.VMEM((count * rank, 3 * rank), F32)]
        + [pltpu.SemaphoreType.DMA((rows // rank, count + 3))]
        + [pltpu.VMEM((rows, rank), F32)] * (count + 3),
        cost_estimate=pl.CostEstimate(
            flops=count * 18 * rows * rank * rank, bytes_accessed=4 * rows * rank * (count + 3), transcendentals=0
        ),
        compiler_params=pltpu.CompilerParams(vmem_limit_bytes=52 * 1024 * 1024),
    )(core, *columns, *panels)


def fro2(value):
    return jnp.sum(value * value)


def inverse_into(n_ref, y_ref, e_ref):
    rank = n_ref.shape[0]
    row = lax.broadcasted_iota(jnp.int32, (rank, rank), 0)
    col = lax.broadcasted_iota(jnp.int32, (rank, rank), 1)
    ident = jnp.where(row == col, 1.0, 0.0).astype(F32)
    y_ref[...] = ident + n_ref[...]
    e_ref[...] = n_ref[...]

    for _ in range(2):
        some = e_ref[...].astype(jnp.bfloat16)
        square = dot(some, some)
        e_ref[...] = square
        y = y_ref[...]
        y_ref[...] = y + dot(y.astype(jnp.bfloat16), square.astype(jnp.bfloat16))

    def residual():
        y = y_ref[...]
        left = ident - y + mm3(cut(y), cut(n_ref[...]))
        e_ref[...] = left
        return fro2(left)

    def improve():
        y = y_ref[...]
        y_ref[...] = y + mm3(cut(e_ref[...]), cut(y))

    size = residual()
    good = size < 0.25

    @pl.when(jnp.logical_not(good))
    def _():
        system = ident - n_ref[...]
        most = jnp.max(jnp.sum(jnp.abs(system), axis=0, keepdims=True))
        most = most * jnp.max(jnp.sum(jnp.abs(system), axis=1, keepdims=True))
        y_ref[...] = jnp.transpose(system) / most
        residual()

    def unfinished(state):
        count, now, before = state
        stuck = jnp.logical_and(now < 0.1, now > 0.25 * before)
        return jnp.logical_and(count < 120, jnp.logical_not(jnp.logical_or(now < 4e-6, stuck)))

    def better(state):
        count, now, _ = state
        improve()
        return count + 1, residual(), now

    lax.while_loop(unfinished, better, (jnp.int32(0), jnp.where(good, size, F32(1e30)), F32(1e35)))
    improve()


def couple_of(spots):
    own = jnp.transpose(spots)
    total = None
    for d in range(3):
        spread = own[:, d : d + 1] - spots[3 + d : 4 + d, :]
        total = spread * spread if total is None else total + spread * spread
    return jnp.exp(-0.5 * total)


def place(core_ref, mine_ref, theirs_ref, full_ref):
    half = mine_ref.shape[0]
    core = core_ref[0]
    full_ref[pl.ds(pl.multiple_of(core * half, half), half), :] = mine_ref[...]
    full_ref[pl.ds(pl.multiple_of((1 - core) * half, half), half), :] = theirs_ref[...]


def spots_of(mine_ref, theirs_ref, at):
    rank = 2 * mine_ref.shape[0]
    total = None
    for ref in (mine_ref, theirs_ref):
        for q in range(rank // 16):
            some = ref[q * 8 : q * 8 + 8, at : at + rank]
            total = some if total is None else total + some
    return total


def level_kernel(at, core_ref, mine_ref, theirs_ref, own_ref, other_ref, ans_ref, next_ref, full, n, y, e):
    rank = full.shape[0]
    gram_at, upper_at, upper, gram_o_at, spot_at = at
    place(core_ref, mine_ref, theirs_ref, full)
    couple = couple_of(spots_of(mine_ref, theirs_ref, spot_at))
    couple_t = jnp.transpose(couple)
    gram = full[:, gram_at : gram_at + rank]
    gram_o = full[:, gram_o_at : gram_o_at + rank]
    c, c_t = cut(couple), cut(couple_t)
    far = cut(mm3(cut(gram_o), c_t))
    n[...] = mm3(cut(mm3(cut(gram), c)), far)
    inverse_into(n, y, e)
    target = mm3(cut(other_ref[...]), c_t) - mm3(cut(mm3(cut(own_ref[:, :rank]), c)), far)
    ans = mm3(cut(target), cut(y[...]))
    ans_ref[...] = ans
    next_ref[...] = own_ref[:, rank : rank + upper] - mm3(cut(ans), cut(full[:, upper_at : upper_at + upper]))


def solve_kernel(at, core_ref, mine_ref, theirs_ref, couple_ref, far_ref, y_ref, *refs):
    full, n, e = refs[-3:]
    rank = full.shape[0]
    gram_at, upper_at, upper, gram_o_at, spot_at = at
    place(core_ref, mine_ref, theirs_ref, full)
    couple = couple_of(spots_of(mine_ref, theirs_ref, spot_at))
    far = mm3(cut(full[:, gram_o_at : gram_o_at + rank]), cut(jnp.transpose(couple)))
    n[...] = mm3(cut(mm3(cut(full[:, gram_at : gram_at + rank]), cut(couple))), cut(far))
    couple_ref[...] = couple
    far_ref[...] = far
    if upper:
        refs[0][...] = full[:, upper_at : upper_at + upper]
    inverse_into(n, y_ref, e)


def call_solve(core, mine, theirs, at):
    rank, upper = 2 * mine.shape[0], at[2]
    vm = pl.BlockSpec(memory_space=pltpu.VMEM)
    square = jax.ShapeDtypeStruct((rank, rank), F32)
    tail = (jax.ShapeDtypeStruct((rank, upper), F32),) if upper else ()
    return pl.pallas_call(
        functools.partial(solve_kernel, at),
        out_shape=(square,) * 3 + tail,
        in_specs=[pl.BlockSpec(memory_space=pltpu.SMEM), vm, vm],
        out_specs=(vm,) * (3 + len(tail)),
        scratch_shapes=[pltpu.VMEM((rank, mine.shape[1]), F32)] + [pltpu.VMEM((rank, rank), F32)] * 2,
        cost_estimate=pl.CostEstimate(
            flops=60 * 2 * rank**3, bytes_accessed=4 * rank * mine.shape[1], transcendentals=rank * rank
        ),
        compiler_params=pltpu.CompilerParams(vmem_limit_bytes=16 * 1024 * 1024),
    )(core, mine, theirs)


def apply_kernel(couple_ref, far_ref, y_ref, up_ref, own_ref, other_ref, ans_ref, next_ref):
    rank = couple_ref.shape[0]
    couple = couple_ref[...]
    near = mm3(cut(own_ref[:, :rank]), cut(couple))
    target = mm3(cut(other_ref[...]), cut(couple), dot_t) - mm3(cut(near), cut(far_ref[...]))
    ans = mm3(cut(target), cut(y_ref[...]))
    ans_ref[...] = ans
    next_ref[...] = own_ref[:, rank:] - mm3(cut(ans), cut(up_ref[...]))


def call_apply(solved, own, other):
    rank, upper = solved[3].shape
    rows = own.shape[0]
    vm = pl.BlockSpec(memory_space=pltpu.VMEM)
    return pl.pallas_call(
        apply_kernel,
        out_shape=(
            jax.ShapeDtypeStruct((rows, rank), F32),
            jax.ShapeDtypeStruct((rows, upper), F32),
        ),
        in_specs=[vm] * 6,
        out_specs=(vm, vm),
        cost_estimate=pl.CostEstimate(
            flops=30 * 2 * rows * rank**2, bytes_accessed=4 * rank * (3 * rank + upper), transcendentals=0
        ),
        compiler_params=pltpu.CompilerParams(vmem_limit_bytes=16 * 1024 * 1024),
    )(*solved, own, other)


def call_level(core, mine, theirs, own, other, at):
    rank = 2 * mine.shape[0]
    rows, upper = own.shape[0], at[2]
    vm = pl.BlockSpec(memory_space=pltpu.VMEM)
    return pl.pallas_call(
        functools.partial(level_kernel, at),
        out_shape=(
            jax.ShapeDtypeStruct((rows, rank), F32),
            jax.ShapeDtypeStruct((rows, upper), F32),
        ),
        in_specs=[pl.BlockSpec(memory_space=pltpu.SMEM), vm, vm, vm, vm],
        out_specs=(vm, vm),
        scratch_shapes=[pltpu.VMEM((rank, mine.shape[1]), F32)] + [pltpu.VMEM((rank, rank), F32)] * 3,
        cost_estimate=pl.CostEstimate(
            flops=80 * 2 * rank**3, bytes_accessed=4 * rank * mine.shape[1], transcendentals=rank * rank
        ),
        compiler_params=pltpu.CompilerParams(vmem_limit_bytes=16 * 1024 * 1024),
    )(core, mine, theirs, own, other)


def top_kernel(core_ref, couple_ref, far_ref, y_ref, mine_ref, theirs_ref, *refs):
    held, out_ref = refs[:4], refs[4]
    full, stacked, result, go = refs[5:]
    rank = full.shape[0]
    place(core_ref, mine_ref, theirs_ref, full)
    part = lambda k: full[:, k * rank : (k + 1) * rank]
    couple = couple_ref[...]
    near = mm3(cut(part(0)), cut(couple))
    target = mm3(cut(part(1)), cut(couple), dot_t) - mm3(cut(near), cut(far_ref[...]))
    top = cut(mm3(cut(target), cut(y_ref[...])))
    mid = cut(part(3) - mm3(top, cut(part(2))))
    low = cut(part(6) - mm3(top, cut(part(5))) - mm3(mid, cut(part(4))))
    for k, (one, two) in enumerate((top, mid, low)):
        stacked[0, :, k * rank : (k + 1) * rank] = one
        stacked[1, :, k * rank : (k + 1) * rank] = two
    rows = result.shape[0]
    chunk = rows // 4
    stores = []
    for i in range(4):
        at = slice(i * chunk, (i + 1) * chunk)
        sides = [cut(held[1 + k][at, :]) for k in range(3)]
        side = tuple(jnp.concatenate(part, 1) for part in zip(*sides))
        total = held[0][at, :] - mm3(side, (stacked[0], stacked[1]), dot_t)
        result[at, :] = total
        store = pltpu.make_async_copy(result.at[at, :], out_ref.at[at, :], go.at[i])
        store.start()
        stores.append(store)
    for store in stores:
        store.wait()


def call_top(core, solved, mine, theirs, carry):
    rank = 2 * mine.shape[0]
    rows = carry[0].shape[0]
    vm = pl.BlockSpec(memory_space=pltpu.VMEM)
    far = pl.BlockSpec(memory_space=pltpu.HBM)
    return pl.pallas_call(
        top_kernel,
        out_shape=jax.ShapeDtypeStruct((rows, rank), F32),
        in_specs=[pl.BlockSpec(memory_space=pltpu.SMEM)] + [vm] * 9,
        out_specs=far,
        scratch_shapes=[pltpu.VMEM((rank, mine.shape[1]), F32)]
        + [pltpu.VMEM((2, rank, 3 * rank), jnp.bfloat16), pltpu.VMEM((rows, rank), F32)]
        + [pltpu.SemaphoreType.DMA((4,))],
        cost_estimate=pl.CostEstimate(
            flops=100 * 2 * rank**3, bytes_accessed=4 * rank * mine.shape[1] + 20 * rows * rank, transcendentals=rank * rank
        ),
        compiler_params=pltpu.CompilerParams(vmem_limit_bytes=32 * 1024 * 1024),
    )(core, *solved, mine, theirs, *carry)


def swap(value, mask):
    count = lax.axis_size("leaf")
    return lax.ppermute(value, "leaf", [(i, i ^ mask) for i in range(count)])


def to_all(piece):
    return jnp.broadcast_to(piece, (lax.axis_size("pts"), *piece.shape))


def exchanged(pieces):
    return lax.all_to_all(pieces, "pts", 0, 0, tiled=True)


def spread_to_all(piece):
    return exchanged(to_all(piece)).reshape(-1, piece.shape[-1])


def per_device(
    leaf_solved,
    points,
    panel_top,
    panel_mid,
    panel_low,
    solved_top,
    solved_mid,
    solved_low,
    skeleton_top,
    skeleton_mid,
    skeleton_low,
):
    rows, rank = panel_top.shape
    many = lax.axis_size("pts")
    leaf = lax.axis_index("leaf")
    core, plane = leaf % 2, leaf // 2
    device = leaf * many + lax.axis_index("pts")
    core_arg = core.astype(jnp.int32).reshape(1)
    panels = (panel_low, panel_mid, panel_top)
    zero2 = jnp.zeros((2, rank), F32)
    each = rank // (2 * many)

    keep, send = call_product(core_arg, (solved_low, solved_mid), panels, many)
    both = exchanged(keep + swap(send, 1)).sum(axis=0)
    first, middle = both[:, : 3 * rank], both[:, 3 * rank :]
    keep, send = call_product(core_arg, (solved_top, leaf_solved), panels, many)
    rest = keep + swap(send, 1)
    take = lambda table, k: lax.dynamic_index_in_dim(table, k, 0, keepdims=False)
    listed = jnp.concatenate(
        [take(skeleton_low, plane), take(skeleton_mid, plane // 2), take(skeleton_top, plane // 4)]
    )
    offsets = listed - device * rows
    select = (offsets[:, None] == jnp.arange(rows, dtype=jnp.int32)[None, :]).astype(F32)
    picked = jnp.einsum("cr,sr->cs", points, select, precision=BEST)
    pick_low, pick_mid, pick_top = (picked[:, k * rank : (k + 1) * rank] for k in range(3))

    mark = jnp.concatenate([pick_low, jnp.zeros((5, rank), F32)], 0)
    first_o = swap(jnp.concatenate([first[:, :rank], mark], 1), 2)
    spots = jnp.concatenate([pick_low, first_o[:3, rank:], zero2], 0)
    piece = jnp.concatenate([first, first_o[:, :rank], spots], 1)
    wide = piece.shape[1]
    got = exchanged(jnp.concatenate([to_all(piece), rest], 2))
    mine = got[:, :, :wide].reshape(-1, wide)
    theirs = swap(mine, 1)
    rest = got[:, :, wide:].sum(axis=0)
    own = jnp.concatenate([middle, rest[:, : 3 * rank], rest[:, 3 * rank :]], 0)
    other = swap(own[:, :rank], 2)
    solved = call_solve(core_arg, mine, theirs, (0, rank, 2 * rank, 3 * rank, 4 * rank))
    low, mid = call_apply(solved, own, other)

    marks = jnp.concatenate([pick_mid, pick_top, zero2], 0)
    mid = jnp.concatenate([mid, jnp.concatenate([marks, jnp.zeros_like(marks)], 1)], 0)
    part = mid[:, :rank]
    near, far1, far2 = swap(mid, 2), swap(part, 4), swap(part, 6)
    mid, mid_o = mid + near, far1 + far2
    marks, marks_o = mid[3 * each :, :rank], mid_o[3 * each :]
    spots = jnp.concatenate([marks[:3], marks_o[:3], zero2], 0)
    marks = marks + marks_o
    mine = spread_to_all(jnp.concatenate([mid[:each], mid_o[:each], spots], 1))
    theirs = swap(mine, 1)
    ans, top = call_level(
        core_arg, mine, theirs, mid[each : 3 * each], mid_o[each : 3 * each], (0, rank, rank, 2 * rank, 3 * rank)
    )

    far1, far2 = swap(jnp.concatenate([top, marks], 0), 8), swap(top, 12)
    top, top_o = top + swap(top, 4), far1[: 2 * each] + far2
    spots = jnp.concatenate([marks[3:6], far1[2 * each + 3 : 2 * each + 6], zero2], 0)
    blocks = [top[:each], top_o[:each], spots, top[each:], top_o[each:]]
    blocks += [ans[:each], ans[each:], low[:each], low[each : 2 * each], low[2 * each :]]
    mine = spread_to_all(jnp.concatenate(blocks, 1))
    early, late = mine[:, : 3 * rank], mine[:, 3 * rank :]
    early_o = swap(early, 1)
    late_o = swap(late, 1)
    solved = call_solve(core_arg, early, early_o, (0, 0, 0, rank, 2 * rank))
    return call_top(core_arg, solved, late, late_o, (leaf_solved, solved_top, solved_mid, solved_low))


def solution(mesh):
    split = P(("leaf", "pts"), None)
    in_specs = (split, P(None, ("leaf", "pts")), *[split] * 6, P(), P(), P())

    return jax.shard_map(per_device, mesh=mesh, in_specs=in_specs, out_specs=split, check_vma=False)
```
